32 devices in a mesh: lat: 8 (over z, x), lev: 4 (over y, core).
Axes of the slice: x: 2, y: 2, z: 4, core: 2. Of those that a mesh axis runs over, the one named last changes fastest.
Arguments:
- fourier: bfloat16 [1280, 640, 1024], P('lat', None, 'lev'), may hold values from -6 to 6
- legendre: bfloat16 [640, 2, 640, 320], P('lat', None, 'lev'), may hold values from -0.25 to 0.25
- owner: int32 [640], replicated, may hold values from 0 to 7, as said below
Outputs:
- spectral: bfloat16 [640, 2, 320, 1024], P('lat', None, None, 'lev')
The draws below stay inside these ranges and needn't reach their ends.
Inputs may be any that keep to these rules, and one draw needn't show every extreme that they name: `owner`: each index along lat is named by exactly 80 wavenumbers.
All inputs are finite; a program needn't handle non-finite values.
Results may differ from the reference program's by a relative error of at most 0.0051.
Values may be sent and summed in bfloat16 or wider, within the bound.
A program may use at most 384 MiB of HBM per device.

```python
import jax
import jax.numpy as jnp
from jax import lax

M = 640
NLAT = 1280
COLS = 1024
NH = 640
HALF = 320
SLOTS = 80
N_LAT = 8


def draw_owner(key, part):
    jitter_key = jax.random.fold_in(key, 101)
    device_key = jax.random.fold_in(key, 202)
    wave_ids = jnp.arange(M, dtype=jnp.int32)
    jitter = jax.random.randint(jitter_key, (M,), 0, 4 * SLOTS, dtype=jnp.int32)
    scores = (wave_ids + jitter) * M + wave_ids
    ordering = jnp.argsort(scores, stable=True).astype(jnp.int32)
    ranking = jnp.argsort(ordering, stable=True).astype(jnp.int32)
    devices = jax.random.permutation(device_key, M // SLOTS).astype(jnp.int32)
    return devices[ranking // SLOTS]


def levels(own_key, extent, split, smallest, high):
    def one(axis_at, shards_of):
        draws = jax.random.uniform(jax.random.fold_in(jax.random.fold_in(own_key, 6), axis_at), (shards_of,), jnp.float32, smallest / len(split), high / len(split))
        return jnp.repeat(jnp.exp(draws), extent[axis_at] // shards_of).reshape((-1,) + (1,) * (len(extent) - axis_at - 1))

    level = one(*split[0])
    for cut in split[1:]:
        level = level * one(*cut)
    return level


def bell_draw(key, dims, scale, reach, shards=(), kind=jnp.bfloat16):
    result = jax.random.normal(key, dims, jnp.float32) * scale
    if len(shards) > 0:
        result = levels(key, dims, shards, -0.22, 0.18) * result
    return jnp.clip(result, min=-reach, max=reach).astype(kind)


def setup_inputs(seed: int = 0) -> dict:
    arg_keys = jax.random.split(jax.random.key(seed), 4)
    fourier = bell_draw(arg_keys[0], (NLAT, M, COLS), 1.0, 6.0, ((0, 8), (2, 4)))
    legendre = bell_draw(arg_keys[1], (M, 2, NH, HALF), NH ** -0.5, 0.25, ((0, 8), (2, 4)))
    owner = draw_owner(jax.random.fold_in(arg_keys[3], 71), 0)
    return {"fourier": fourier, "legendre": legendre, "owner": owner}


def slot_waves(owner, slot_count):
    wave_count = owner.shape[0]
    wave_ids = jnp.arange(wave_count, dtype=jnp.int32)
    earlier = (owner[None, :] == owner[:, None]) & (wave_ids[None, :] < wave_ids[:, None])
    ranked = jnp.sum(earlier.astype(jnp.int32), axis=1)
    placed = owner * slot_count + ranked
    matched = placed[None, :] == wave_ids[:, None]
    return jnp.sum(jnp.where(matched, wave_ids[None, :], 0), axis=1).astype(jnp.int32)


def reference(fourier, legendre, owner):
    wave_of = slot_waves(owner, M // N_LAT)
    north_count = NLAT // 2
    degree = jnp.arange(M // 2, dtype=jnp.int32)
    parities = jnp.arange(2, dtype=jnp.int32)

    def one_slot(operands):
        wave, table_part = operands
        column = lax.dynamic_index_in_dim(fourier, wave, axis=1, keepdims=False)
        upper_rows = column[:north_count].astype(jnp.float32)
        lower_rows = column[north_count:].astype(jnp.float32)
        even_rows = (upper_rows + lower_rows).astype(jnp.bfloat16)
        odd_rows = (upper_rows - lower_rows).astype(jnp.bfloat16)
        even_out = jnp.dot(table_part[0].T, even_rows, preferred_element_type=jnp.float32)
        odd_out = jnp.dot(table_part[1].T, odd_rows, preferred_element_type=jnp.float32)
        live_count = (M - wave - parities + 1) // 2
        kept_mask = degree[None, :] < live_count[:, None]
        stacked = jnp.stack([even_out, odd_out])
        return jnp.where(kept_mask[:, :, None], stacked, 0.0).astype(jnp.bfloat16)

    return lax.map(one_slot, (wave_of, legendre))
```

```python
import functools

import jax
import jax.numpy as jnp
from jax import lax
from jax.experimental import pallas as pl
from jax.experimental.pallas import tpu as pltpu
from jax.sharding import PartitionSpec as P

CHUNKS = 2


def slot_places(owner, slot_count):
    wave_count = owner.shape[0]
    wave_ids = jnp.arange(wave_count, dtype=jnp.int32)
    earlier = (owner[None, :] == owner[:, None]) & (wave_ids[None, :] < wave_ids[:, None])
    ranked = jnp.sum(earlier.astype(jnp.int32), axis=1)
    placed = owner * slot_count + ranked
    return placed[None, :] == wave_ids[:, None]


def project(base, wave_count, waves_ref, rows_ref, table_ref, *rest):
    out_ref = rest[-1]
    half_rows, column_count = out_ref.shape[2:]
    half = rows_ref.shape[0] // 2
    upper = rows_ref[:half, 0].astype(jnp.float32).reshape(-1, column_count)
    lower = rows_ref[half:, 0].astype(jnp.float32).reshape(-1, column_count)
    wave = waves_ref[base + pl.program_id(0)]
    degree = lax.broadcasted_iota(jnp.int32, (half_rows, column_count), 0)
    for parity in range(2):
        part = (upper + lower if parity == 0 else upper - lower).astype(jnp.bfloat16)
        total = lax.dot_general(
            table_ref[0, parity], part, (((0,), (0,)), ((), ())),
            preferred_element_type=jnp.float32,
        )
        live = (wave_count - wave - parity + 1) // 2
        out_ref[0, parity] = jnp.where(degree < live, total, 0.0).astype(out_ref.dtype)


def project_chunk(base, wave_count, own_waves, rows, table, previous):
    groups, chunk_slots, group_rows, column_count = rows.shape
    slot_count, _, north_count, half_rows = table.shape
    in_specs = [
        pl.BlockSpec((groups, 1, group_rows, column_count), lambda s, w: (0, s, 0, 0)),
        pl.BlockSpec((1, 2, north_count, half_rows), lambda s, w: (base + s, 0, 0, 0)),
    ]
    operands = [own_waves, rows, table]
    aliases = {}
    if previous is not None:
        in_specs.append(pl.BlockSpec(memory_space=pl.ANY))
        operands.append(previous)
        aliases = {3: 0}
    return pl.pallas_call(
        functools.partial(project, base, wave_count),
        grid_spec=pltpu.PrefetchScalarGridSpec(
            num_scalar_prefetch=1,
            grid=(chunk_slots,),
            in_specs=in_specs,
            out_specs=pl.BlockSpec(
                (1, 2, half_rows, column_count), lambda s, w: (base + s, 0, 0, 0)
            ),
        ),
        out_shape=jax.ShapeDtypeStruct(
            (slot_count, 2, half_rows, column_count), jnp.bfloat16
        ),
        input_output_aliases=aliases,
        compiler_params=pltpu.CompilerParams(vmem_limit_bytes=32 * 1024 * 1024),
        cost_estimate=pl.CostEstimate(
            flops=4 * chunk_slots * north_count * half_rows * column_count,
            bytes_accessed=2 * rows.size
            + 4 * chunk_slots * half_rows * (north_count + column_count),
            transcendentals=0,
        ),
    )(*operands)


def body(fourier, legendre, owner):
    lat_count = lax.axis_size("lat")
    row_count, wave_count, column_count = fourier.shape
    slot_count = wave_count // lat_count
    matched = slot_places(owner, slot_count)
    wave_ids = jnp.arange(wave_count, dtype=jnp.int32)
    wave_of = jnp.sum(jnp.where(matched, wave_ids[None, :], 0), axis=1)
    own_waves = lax.dynamic_slice_in_dim(wave_of, lax.axis_index("lat") * slot_count, slot_count)
    table = lax.all_gather(legendre, "lev", axis=2, tiled=True)
    picks = matched.astype(jnp.bfloat16).reshape(lat_count, slot_count, wave_count)
    chunks = CHUNKS if slot_count % CHUNKS == 0 else 1
    chunk_slots = slot_count // chunks
    result = None
    for chunk in range(chunks):
        base = chunk * chunk_slots
        pick = picks[:, base : base + chunk_slots].reshape(-1, wave_count)
        outgoing = lax.dot_general(
            pick, fourier, (((1,), (1,)), ((), ())), preferred_element_type=jnp.bfloat16
        )
        arrived = lax.all_to_all(outgoing, "lat", split_axis=0, concat_axis=0, tiled=True)
        arrived = arrived.reshape(lat_count, chunk_slots, row_count, column_count)
        if row_count % 16 != 0:
            arrived = arrived.reshape(2, lat_count // 2, chunk_slots, row_count, column_count)
            arrived = arrived.swapaxes(1, 2).reshape(2, chunk_slots, -1, column_count)
        result = project_chunk(base, wave_count, own_waves, arrived, table, result)
    return result


def solution(mesh):
    placed = (P("lat", None, "lev"), P("lat", None, "lev", None), P())
    return jax.shard_map(
        body, mesh=mesh, in_specs=placed, out_specs=P("lat", None, None, "lev"), check_vma=False
    )
```
